8 devices in a mesh: dp: 1 (over z), cp: 2 (over y), tp: 4 (over x, core).
Axes of the slice: x: 2, y: 2, z: 1, core: 2. Of those that a mesh axis runs over, the one named last changes fastest.
Arguments:
- x: bfloat16 [2048, 4096], P(('dp', 'cp', 'tp'))
- idx: int32 [2048, 2], P(('dp', 'cp', 'tp'))
- gates: float32 [2048, 2], P(('dp', 'cp', 'tp'))
- wq: bfloat16 [4096, 4096], P(None, 'tp')
- wk: bfloat16 [4096, 1024], P(None, 'tp')
- wv: bfloat16 [4096, 1024], P(None, 'tp')
- wo: bfloat16 [4096, 4096], P('tp')
- w1g: bfloat16 [8, 4096, 6400], P(('cp', 'tp'))
- w1u: bfloat16 [8, 4096, 6400], P(('cp', 'tp'))
- w2: bfloat16 [8, 6400, 4096], P(('cp', 'tp'))
Outputs:
- output: bfloat16 [2048, 4096], P(('dp', 'cp', 'tp'))
All inputs are finite; a program needn't handle non-finite values.
Results may differ from the reference program's by a relative error of at most 0.00893337.
Values are sent between devices in bfloat16 or wider.
A program may use at most 1 GiB of HBM per device.

```python
import math
import jax
import jax.numpy as jnp
from jax import lax

H = 4096
FF = 6400
HEADS = 32
KV_HEADS = 8
HEAD = 128
S = 2048
CP = 2
TP = 4
TOP = 2
QBLK = 512

E = CP * TP
T = S // E
CAP = 4 * T // E
M = 2 * T // E


def seg_positions():
    i = jnp.arange(S, dtype=jnp.int32)
    seg = S // (2 * CP)
    b = i // seg
    r = b // 2
    s_id = jnp.where(b % 2 == 0, r, 2 * CP - 1 - r)
    return s_id * seg + i % seg


def source_routing(key, sigma, counts):
    ends = jnp.cumsum(counts)
    labels = sigma[jnp.searchsorted(ends, jnp.arange(2 * T, dtype=jnp.int32), side='right')]
    perm = jax.random.permutation(key, T)
    return jnp.stack([labels[perm], labels[perm + T]], axis=1).astype(jnp.int32)


def setup_inputs(seed: int = 0, part: int = 0) -> dict:
    key = jax.random.key(seed)
    ks = jax.random.split(key, 7)
    kx = jax.random.split(jax.random.fold_in(key, part), 4)
    a = math.log(S / 16.0) ** 0.25

    def nrm(k, shape, scale):
        return (jax.random.normal(k, shape, jnp.float32) * scale).astype(jnp.bfloat16)

    wq = nrm(ks[0], (H, HEADS * HEAD), a / math.sqrt(H))
    wk = nrm(ks[1], (H, KV_HEADS * HEAD), a / math.sqrt(H))
    wv = nrm(ks[2], (H, KV_HEADS * HEAD), 1.0 / math.sqrt(H))
    wo = nrm(ks[3], (HEADS * HEAD, H), 1.0 / math.sqrt(HEADS * HEAD))
    w1g = nrm(ks[4], (E, H, FF), 1.0 / math.sqrt(H))
    w1u = nrm(ks[5], (E, H, FF), 1.0 / math.sqrt(H))
    w2 = nrm(ks[6], (E, FF, H), 1.5 / math.sqrt(FF))
    x = nrm(kx[0], (S, H), 1.0)
    sigmas = jax.vmap(lambda kk: jax.random.permutation(kk, E))(jax.random.split(kx[1], E))
    counts = jnp.full((E,), M, jnp.int32)
    idx = jax.vmap(lambda kk, sg: source_routing(kk, sg, counts))(jax.random.split(kx[2], E), sigmas)
    idx = idx.reshape(S, TOP)
    gates = jax.random.uniform(kx[3], (S, TOP), jnp.float32, 0.3, 0.7)
    return {'x': x, 'idx': idx, 'gates': gates, 'wq': wq, 'wk': wk, 'wv': wv, 'wo': wo, 'w1g': w1g, 'w1u': w1u, 'w2': w2}


def reference(x, idx, gates, wq, wk, wv, wo, w1g, w1u, w2):
    pos = seg_positions()
    g = HEADS // KV_HEADS
    q = jnp.dot(x, wq, preferred_element_type=jnp.float32).astype(jnp.bfloat16)
    k = jnp.dot(x, wk, preferred_element_type=jnp.float32).astype(jnp.bfloat16)
    v = jnp.dot(x, wv, preferred_element_type=jnp.float32).astype(jnp.bfloat16)
    qh = q.reshape(S, HEADS, HEAD).transpose(1, 0, 2)
    kh = jnp.repeat(k.reshape(S, KV_HEADS, HEAD).transpose(1, 0, 2), g, axis=0)
    vh = jnp.repeat(v.reshape(S, KV_HEADS, HEAD).transpose(1, 0, 2), g, axis=0)
    scale = HEAD ** -0.5
    nb = S // QBLK

    def head(args):
        qa, ka, va = args

        def block(bargs):
            qb, pb = bargs
            s = jnp.dot(qb, ka.T, preferred_element_type=jnp.float32) * scale
            mask = pos[None, :] <= pb[:, None]
            s = jnp.where(mask, s, -1e30)
            m = jnp.max(s, axis=-1, keepdims=True)
            w = jnp.where(mask, jnp.exp(s - m), 0.0)
            l = jnp.sum(w, axis=-1, keepdims=True)
            ob = jnp.dot(w.astype(jnp.bfloat16), va, preferred_element_type=jnp.float32)
            return ob / l

        out = lax.map(block, (qa.reshape(nb, QBLK, HEAD), pos.reshape(nb, QBLK)))
        return out.reshape(S, HEAD)

    o = lax.map(head, (qh, kh, vh))
    o = o.transpose(1, 0, 2).reshape(S, HEADS * HEAD).astype(jnp.bfloat16)
    att = jnp.dot(o, wo, preferred_element_type=jnp.float32)
    h = (x.astype(jnp.float32) + att).astype(jnp.bfloat16)

    ea = idx.reshape(-1)
    tok = jnp.arange(S * TOP) // TOP
    onehot = (ea[:, None] == jnp.arange(E)[None, :]).astype(jnp.int32)
    slot = jnp.take_along_axis(jnp.cumsum(onehot, axis=0), ea[:, None], axis=1)[:, 0] - 1
    ct = E * CAP
    buf = jnp.zeros((E, ct, H), jnp.bfloat16).at[ea, slot].set(h[tok])

    def expert(args):
        rows, wg, wu, wd = args
        gg = jnp.dot(rows, wg, preferred_element_type=jnp.float32)
        uu = jnp.dot(rows, wu, preferred_element_type=jnp.float32)
        act = (jax.nn.silu(gg) * uu).astype(jnp.bfloat16)
        return jnp.dot(act, wd, preferred_element_type=jnp.float32).astype(jnp.bfloat16)

    z = lax.map(expert, (buf, w1g, w1u, w2))
    zt = z[ea, slot].astype(jnp.float32).reshape(S, TOP, H)
    y = h.astype(jnp.float32) + jnp.sum(gates[:, :, None] * zt, axis=1)
    return y.astype(jnp.bfloat16)
```

```python
import functools

import jax
import jax.numpy as jnp
from jax import lax
from jax.experimental import pallas as pl
from jax.experimental.pallas import tpu as pltpu
from jax.sharding import PartitionSpec as P

HEAD_DIM = 128
NEG = -1e30
LOG2E = 1.4426950408889634
MESH = pl.DeviceIdType.MESH
BF = jnp.bfloat16
F32 = jnp.float32
VMEM_LIMIT = 60 * 1024 * 1024


def attn_body(rank_ref, q_ref, k_ref, v_ref, o_ref, *, seg, cp, bq, scale):
    rank = rank_ref[0]
    c = scale * LOG2E

    def block(s_id):
        src = jnp.where(s_id < cp, s_id, 2 * cp - 1 - s_id)
        off = jnp.where(s_id < cp, 0, seg)
        return src, pl.multiple_of(off, seg)

    def update(carry, s, vj):
        m, l, acc = carry
        mn = jnp.maximum(m, jnp.max(s, axis=-1, keepdims=True))
        w = jnp.exp2((s - mn) * c)
        a = jnp.exp2((m - mn) * c)
        l = l * a + jnp.sum(w, axis=-1, keepdims=True)
        acc = acc * a + jnp.dot(w.astype(BF), vj, preferred_element_type=F32)
        return mn, l, acc

    def score(q, kj):
        return lax.dot_general(q, kj, (((1,), (1,)), ((), ())), preferred_element_type=F32)

    for half in range(2):
        mine = rank if half == 0 else 2 * cp - 1 - rank
        for r in range(seg // bq):
            rows = pl.ds(half * seg + r * bq, bq)
            q = q_ref[rows, :]
            init = (jnp.full((bq, 1), NEG, F32), jnp.zeros((bq, 1), F32), jnp.zeros((bq, HEAD_DIM), F32))

            def full(j, carry):
                src, off = block(j)
                kj = k_ref[src, pl.ds(off, seg), :]
                vj = v_ref[src, pl.ds(off, seg), :]
                return update(carry, score(q, kj), vj)

            carry = lax.fori_loop(0, mine, full, init)
            src, off = block(mine)
            w = (r + 1) * bq
            kj = k_ref[src, pl.ds(off, w), :]
            vj = v_ref[src, pl.ds(off, w), :]
            s = score(q, kj)
            qi = r * bq + lax.broadcasted_iota(jnp.int32, (bq, w), 0)
            ki = lax.broadcasted_iota(jnp.int32, (bq, w), 1)
            s = jnp.where(ki <= qi, s, NEG)
            m, l, acc = update(carry, s, vj)
            o_ref[rows, :] = (acc / l).astype(BF)


def attention(q, kvs, rank, cp):
    n, wq = q.shape
    heads = wq // HEAD_DIM
    kvh = kvs.shape[2] // (2 * HEAD_DIM)
    g = heads // kvh
    seg = n // 2
    body = functools.partial(attn_body, seg=seg, cp=cp, bq=seg // 2, scale=HEAD_DIM ** -0.5)
    return pl.pallas_call(
        body,
        grid_spec=pltpu.PrefetchScalarGridSpec(
            num_scalar_prefetch=1,
            grid=(heads,),
            in_specs=[
                pl.BlockSpec((n, HEAD_DIM), lambda j, r: (0, j)),
                pl.BlockSpec((cp, n, HEAD_DIM), lambda j, r: (0, 0, j // g)),
                pl.BlockSpec((cp, n, HEAD_DIM), lambda j, r: (0, 0, kvh + j // g)),
            ],
            out_specs=pl.BlockSpec((n, HEAD_DIM), lambda j, r: (0, j)),
        ),
        out_shape=jax.ShapeDtypeStruct((n, wq), BF),
        compiler_params=pltpu.CompilerParams(vmem_limit_bytes=32 * 1024 * 1024),
        cost_estimate=pl.CostEstimate(flops=20_000_000_000, bytes_accessed=8_000_000, transcendentals=10_000_000),
        name='attn',
    )(rank.reshape(1), q, kvs, kvs)


def up_body(x_ref, g_ref, u_ref, a_ref):
    x = x_ref[...]
    gg = jnp.dot(x, g_ref[0], preferred_element_type=F32)
    uu = jnp.dot(x, u_ref[0], preferred_element_type=F32)
    a_ref[...] = (jax.nn.silu(gg) * uu).astype(BF)


def expert_up(rows, wg, wu, tile):
    r, hd = rows.shape
    ff = wg.shape[2]
    return pl.pallas_call(
        up_body,
        grid=(ff // tile,),
        in_specs=[
            pl.BlockSpec((r, hd), lambda j: (0, 0)),
            pl.BlockSpec((1, hd, tile), lambda j: (0, 0, j)),
            pl.BlockSpec((1, hd, tile), lambda j: (0, 0, j)),
        ],
        out_specs=pl.BlockSpec((r, tile), lambda j: (0, j)),
        out_shape=jax.ShapeDtypeStruct((r, ff), BF),
        compiler_params=pltpu.CompilerParams(vmem_limit_bytes=VMEM_LIMIT),
        cost_estimate=pl.CostEstimate(flops=4 * r * hd * ff, bytes_accessed=4 * hd * ff, transcendentals=r * ff),
        name='expert_up',
    )(rows, wg, wu)


def down_body(a_ref, w_ref, h_ref, tgt_ref, gate_ref, y_ref, zs, zb, send_sem, recv_sem, own_sem, *, cp, tp, cap, nt, lag):
    step = pl.program_id(0)
    ne = cp * tp
    c = lax.axis_index('cp')
    t = lax.axis_index('tp')
    me = c * tp + t

    def peer(d):
        return {'cp': c ^ (d // tp), 'tp': t ^ (d % tp)}, (c ^ (d // tp)) * tp + (t ^ (d % tp))

    def rows(e):
        return pl.ds(pl.multiple_of(e * cap, cap), cap)

    def remote(n, d):
        where, e = peer(d)
        return pltpu.make_async_remote_copy(
            src_ref=zs.at[n, rows(e)], dst_ref=zb.at[n, rows(me)], send_sem=send_sem.at[n, d],
            recv_sem=recv_sem.at[n, d], device_id=where, device_id_type=MESH)

    def own(n):
        return pltpu.make_async_copy(zs.at[n, rows(me)], zb.at[n, rows(me)], own_sem.at[n])

    @pl.when(step == 0)
    def _():
        barrier = pltpu.get_barrier_semaphore()
        for d in range(1, ne):
            pl.semaphore_signal(barrier, inc=1, device_id=peer(d)[0], device_id_type=MESH)
        pl.semaphore_wait(barrier, ne - 1)

    @pl.when((step >= 1) & (step <= nt))
    def _():
        for d in range(1, ne):
            remote(step - 1, d).start()
        own(step - 1).start()

    @pl.when(step < nt)
    def _():
        zs[step] = jnp.dot(a_ref[...], w_ref[0], preferred_element_type=F32).astype(BF)

    @pl.when(step >= lag)
    def _():
        n = step - lag
        own(n).wait()
        for d in range(1, ne):
            remote(n, d).wait_recv()
        slots = lax.broadcasted_iota(jnp.int32, (tgt_ref.shape[0], ne * cap), 1)
        z = zb[n]
        acc = h_ref[...].astype(F32)
        zsum = None
        for k in range(tgt_ref.shape[1]):
            pick = (slots == tgt_ref[:, k:k + 1]).astype(BF)
            zk = gate_ref[:, k:k + 1] * jnp.dot(pick, z, preferred_element_type=F32)
            zsum = zk if zsum is None else zsum + zk
        y_ref[...] = (acc + zsum).astype(BF)
        for d in range(1, ne):
            remote(n, d).wait_send()


def expert_down(act, wd, h, tgt, gates, cp, tp, cap, tile, lag):
    r, ff = act.shape
    t, hd = h.shape
    kk = tgt.shape[1]
    ne = cp * tp
    nt = hd // tile
    body = functools.partial(down_body, cp=cp, tp=tp, cap=cap, nt=nt, lag=lag)
    late = lambda j: (0, jnp.maximum(j - lag, 0))
    return pl.pallas_call(
        body,
        grid=(nt + lag,),
        in_specs=[
            pl.BlockSpec((r, ff), lambda j: (0, 0)),
            pl.BlockSpec((1, ff, tile), lambda j: (0, 0, jnp.minimum(j, nt - 1))),
            pl.BlockSpec((t, tile), late),
            pl.BlockSpec((t, kk), lambda j: (0, 0)),
            pl.BlockSpec((t, kk), lambda j: (0, 0)),
        ],
        out_specs=pl.BlockSpec((t, tile), late),
        out_shape=jax.ShapeDtypeStruct((t, hd), BF),
        scratch_shapes=[
            pltpu.VMEM((nt, r, tile), BF),
            pltpu.VMEM((nt, r, tile), BF),
            pltpu.SemaphoreType.DMA((nt, ne)),
            pltpu.SemaphoreType.DMA((nt, ne)),
            pltpu.SemaphoreType.DMA((nt,)),
        ],
        compiler_params=pltpu.CompilerParams(vmem_limit_bytes=VMEM_LIMIT, collective_id=cap, has_side_effects=True),
        cost_estimate=pl.CostEstimate(flops=2 * r * hd * ff, bytes_accessed=2 * hd * ff, transcendentals=0),
        name='expert_down',
    )(act, wd, h, tgt, gates)


def solution(mesh):
    cp = mesh.shape['cp']
    tp = mesh.shape['tp']
    ne = cp * tp
    rows_spec = P(('dp', 'cp', 'tp'), None)
    exp_spec = P(('cp', 'tp'), None, None)

    def local(x, idx, gates, wq, wk, wv, wo, w1g, w1u, w2):
        t, hd = x.shape
        kk = idx.shape[1]
        rank = lax.axis_index('cp')

        ea = idx.reshape(-1)
        onehot = (ea[:, None] == jnp.arange(ne)[None, :]).astype(jnp.int32)
        cum = jnp.cumsum(onehot, axis=0)
        slot = (jnp.sum(cum * onehot, axis=1) - 1).reshape(t, kk)
        fullest = lax.pmax(jnp.max(cum[-1]), ('cp', 'tp'))

        xs = lax.all_gather(x, 'tp', axis=0, tiled=True)
        k = jnp.dot(xs, wk, preferred_element_type=F32).astype(BF)
        v = jnp.dot(xs, wv, preferred_element_type=F32).astype(BF)
        kvs = lax.all_gather(jnp.concatenate([k, v], axis=1), 'cp', axis=0)
        q = jnp.dot(xs, wq, preferred_element_type=F32).astype(BF)
        o = attention(q, kvs, rank, cp)
        part = jnp.dot(o, wo, preferred_element_type=F32)
        att = lax.psum_scatter(part, 'tp', scatter_dimension=0, tiled=True)
        h = (x.astype(F32) + att).astype(BF)

        def moe(cap):
            def run(h, idx, slot, gates, w1g, w1u, w2):
                tgt = idx * cap + slot
                place = jnp.arange(ne * cap)[:, None]
                pick = ((place == tgt[None, :, 0]) | (place == tgt[None, :, 1])).astype(BF)
                send = jnp.dot(pick, h, preferred_element_type=F32).astype(BF).reshape(ne, cap, hd)
                recv = lax.all_to_all(send, ('cp', 'tp'), 0, 0, tiled=True)
                act = expert_up(recv.reshape(ne * cap, hd), w1g, w1u, 256)
                return expert_down(act, w2, h, tgt, gates, cp, tp, cap, 256, 4)
            return run

        caps = (2 * t // ne, 3 * t // ne, 4 * t // ne)
        tier = (fullest > caps[0]).astype(jnp.int32) + (fullest > caps[1]).astype(jnp.int32)
        return lax.switch(tier, [moe(cap) for cap in caps], h, idx, slot, gates, w1g, w1u, w2)

    return jax.shard_map(local, mesh=mesh, in_specs=(rows_spec, rows_spec, rows_spec, P(None, 'tp'), P(None, 'tp'), P(None, 'tp'), P('tp', None), exp_spec, exp_spec, exp_spec), out_specs=rows_spec, check_vma=False)
```

```python
import functools

import jax
import jax.numpy as jnp
from jax import lax
from jax.experimental import pallas as pl
from jax.experimental.pallas import tpu as pltpu
from jax.sharding import PartitionSpec as P

HEAD_DIM = 128
NEG = -1e30
LOG2E = 1.4426950408889634
MESH = pl.DeviceIdType.MESH
BF = jnp.bfloat16
F32 = jnp.float32
VMEM_LIMIT = 60 * 1024 * 1024


def qkv_body(x_ref, cnt_ref, wq_hbm, wk_hbm, wv_hbm, q_ref, kv_ref, top_ref, wq, wk, wv, near, far, cnts,
             load_sem, psend, precv, xsend, xrecv, fsend, frecv, ksend, krecv, csend, crecv, *, cp, tp, ch):
    c = lax.axis_index('cp')
    t = lax.axis_index('tp')
    rows, hd = x_ref.shape
    part = rows // ch
    wide = q_ref.shape[1]
    kw = wk.shape[1]
    partner, across, other = {'tp': t ^ 1}, {'tp': t ^ 2}, {'cp': 1 - c}

    loads = [pltpu.make_async_copy(s, d, load_sem.at[i]) for i, (s, d) in enumerate(((wk_hbm, wk), (wv_hbm, wv), (wq_hbm, wq)))]
    for ld in loads:
        ld.start()

    def peer(d):
        return {'cp': c ^ (d // tp), 'tp': t ^ (d % tp)}

    barrier = pltpu.get_barrier_semaphore()
    for d in range(1, cp * tp):
        pl.semaphore_signal(barrier, inc=1, device_id=peer(d), device_id_type=MESH)
    pl.semaphore_wait(barrier, cp * tp - 1)

    def copy(src, dst, ss, rs, where):
        return pltpu.make_async_remote_copy(src_ref=src, dst_ref=dst, send_sem=ss, recv_sem=rs, device_id=where, device_id_type=MESH)

    out = [copy(x_ref.at[pl.ds(i * part, part)], far.at[i, 0], xsend.at[i], xrecv.at[i], across) for i in range(ch)]
    fwd = [copy(far.at[i, 0], far.at[i, 1], fsend.at[i], frecv.at[i], partner) for i in range(ch)]
    side = copy(x_ref, near, psend, precv, partner)
    count = [copy(cnt_ref, cnts.at[d], csend.at[d], crecv.at[d], peer(d)) for d in range(1, cp * tp)]
    for cpy in out:
        cpy.start()
    side.start()
    for cpy in count:
        cpy.start()

    def keys(n, first, size):
        sl = (c, pl.ds(pl.multiple_of(first, part), size))
        return copy(kv_ref.at[sl], kv_ref.at[sl], ksend.at[n], krecv.at[n], other)

    def project(xv, pieces, sends):
        def put(ref, val, col, width):
            for a, size, first in pieces:
                ref[pl.ds(pl.multiple_of(first, part), size), pl.ds(col, width)] = val[a:a + size].astype(BF)

        mine = kv_ref.at[c]
        put(mine, jnp.dot(xv, wk[...], preferred_element_type=F32), 0, kw)
        put(mine, jnp.dot(xv, wv[...], preferred_element_type=F32), kw, kw)

        def qtile(j):
            col = pl.multiple_of(j * kw, kw)
            put(q_ref, jnp.dot(xv, wq[:, pl.ds(col, kw)], preferred_element_type=F32), col, kw)

        qtile(0)
        for s in sends:
            s.start()

        @pl.loop(1, wide // kw)
        def _(j):
            qtile(j)

    for ld in loads:
        ld.wait()
    kcopies = []
    k0 = keys(0, t * rows, rows)
    kcopies.append(k0)
    project(x_ref[...], ((0, rows, t * rows),), (k0,))
    side.wait_recv()
    k1 = keys(1, (t ^ 1) * rows, rows)
    kcopies.append(k1)
    project(near[...], ((0, rows, (t ^ 1) * rows),), (k1,))
    for i in range(ch):
        out[i].wait_recv()
        fwd[i].start()
        fwd[i].wait_recv()
        r2 = (t ^ 2) * rows + i * part
        r3 = (t ^ 3) * rows + i * part
        ks = (keys(2 + 2 * i, r2, part), keys(3 + 2 * i, r3, part))
        kcopies.extend(ks)
        project(far[i].reshape(2 * part, hd), ((0, part, r2), (part, part, r3)), ks)
    top = cnt_ref[...]
    for d in range(1, cp * tp):
        count[d - 1].wait()
        top = jnp.maximum(top, cnts[d])
    top_ref[...] = top

    def keys_in(n, first, size):
        sl = (1 - c, pl.ds(pl.multiple_of(first, part), size))
        return copy(kv_ref.at[sl], kv_ref.at[sl], ksend.at[n], krecv.at[n], other)

    keys_in(0, t * rows, rows).wait_recv()
    keys_in(1, (t ^ 1) * rows, rows).wait_recv()
    for i in range(ch):
        keys_in(2 + 2 * i, (t ^ 2) * rows + i * part, part).wait_recv()
        keys_in(3 + 2 * i, (t ^ 3) * rows + i * part, part).wait_recv()
    for kc in kcopies:
        kc.wait_send()
    side.wait_send()
    for i in range(ch):
        out[i].wait_send()
        fwd[i].wait_send()


def project_qkv(x, cnt, wq, wk, wv, cp, tp):
    t, hd = x.shape
    n = t * tp
    wide, kw = wq.shape[1], wk.shape[1]
    ch = 4
    vm = pl.BlockSpec(memory_space=pltpu.VMEM)
    hbm = pl.BlockSpec(memory_space=pl.ANY)
    dma = pltpu.SemaphoreType.DMA
    return pl.pallas_call(
        functools.partial(qkv_body, cp=cp, tp=tp, ch=ch),
        in_specs=[vm, vm, hbm, hbm, hbm],
        out_specs=[vm, vm, vm],
        out_shape=[jax.ShapeDtypeStruct((n, wide), BF), jax.ShapeDtypeStruct((cp, n, 2 * kw), BF), jax.ShapeDtypeStruct(cnt.shape, cnt.dtype)],
        scratch_shapes=[
            pltpu.VMEM(wq.shape, BF), pltpu.VMEM(wk.shape, BF), pltpu.VMEM(wv.shape, BF),
            pltpu.VMEM((t, hd), BF), pltpu.VMEM((ch, 2, t // ch, hd), BF), pltpu.VMEM((cp * tp,) + cnt.shape, cnt.dtype),
            dma((3,)), dma, dma, dma((ch,)), dma((ch,)), dma((ch,)), dma((ch,)),
            dma((2 + 2 * ch,)), dma((2 + 2 * ch,)), dma((cp * tp,)), dma((cp * tp,)),
        ],
        compiler_params=pltpu.CompilerParams(vmem_limit_bytes=VMEM_LIMIT, collective_id=0, has_side_effects=True),
        cost_estimate=pl.CostEstimate(flops=2 * n * hd * (wide + 2 * kw), bytes_accessed=20_000_000, transcendentals=0),
        name='project_qkv',
    )(x, cnt, wq, wk, wv)


def attn_out_body(q_ref, kv_ref, x_ref, wo_hbm, h_ref, wo, ob, pt, rc, sm, rx,
                  load_sem, dsend, drecv, xsend, xrecv, *, cp, tp, nb, tile, scale):
    c = lax.axis_index('cp')
    t = lax.axis_index('tp')
    core, side = t % 2, t // 2
    rows, hd = x_ref.shape
    seg = 2 * rows
    sub = rows // nb
    nt = hd // tile
    heads = q_ref.shape[1] // HEAD_DIM
    kvh = kv_ref.shape[2] // (2 * HEAD_DIM)
    g = heads // kvh
    cc = scale * LOG2E

    load = pltpu.make_async_copy(wo_hbm, wo, load_sem)
    load.start()
    partner, across = {'tp': t ^ 1}, {'tp': t ^ 2}
    barrier = pltpu.get_barrier_semaphore()
    for where in (partner, across):
        pl.semaphore_signal(barrier, inc=1, device_id=where, device_id_type=MESH)
    pl.semaphore_wait(barrier, 2)

    def pass_half(i, n):
        return pltpu.make_async_remote_copy(
            src_ref=pt.at[i % 2, n, 1 - core], dst_ref=rc.at[i, n], send_sem=dsend.at[i % 2, n], recv_sem=drecv.at[i, n],
            device_id=partner, device_id_type=MESH)

    def pass_sum(i):
        return pltpu.make_async_remote_copy(
            src_ref=sm.at[i], dst_ref=rx.at[i], send_sem=xsend.at[i], recv_sem=xrecv.at[i],
            device_id=across, device_id_type=MESH)

    def score(q, kj):
        return lax.dot_general(q, kj, (((1,), (1,)), ((), ())), preferred_element_type=F32)

    def update(state, s, vj):
        m, l, acc = state
        mn = jnp.maximum(m, jnp.max(s, axis=-1, keepdims=True))
        w = jnp.exp2((s - mn) * cc)
        a = jnp.exp2((m - mn) * cc)
        l = l * a + jnp.sum(w, axis=-1, keepdims=True)
        acc = acc * a + jnp.dot(w.astype(BF), vj, preferred_element_type=F32)
        return mn, l, acc

    def block(s_id, width):
        src = jnp.where(s_id < cp, s_id, 2 * cp - 1 - s_id)
        return src, pl.ds(pl.multiple_of(jnp.where(s_id < cp, 0, seg), seg), width)

    def attend(i, half):
        place = jnp.where(i < nb, 1 - side, side)
        s_id = jnp.where(place == 0, c, 2 * cp - 1 - c)
        first = half * rows + (i % nb) * sub
        qrows = pl.ds(pl.multiple_of(place * seg + first, sub), sub)
        m4 = g * sub
        qs = [jnp.concatenate([q_ref[qrows, (a * g + b) * HEAD_DIM:(a * g + b + 1) * HEAD_DIM] for b in range(g)], axis=0)
              for a in range(kvh)]
        state = tuple((jnp.full((m4, 1), NEG, F32), jnp.zeros((m4, 1), F32), jnp.zeros((m4, HEAD_DIM), F32)) for _ in range(kvh))

        def kv(a, s, width):
            src, sl = block(s, width)
            return (kv_ref[src, sl, a * HEAD_DIM:(a + 1) * HEAD_DIM],
                    kv_ref[src, sl, (kvh + a) * HEAD_DIM:(kvh + a + 1) * HEAD_DIM])

        def full(j, state):
            pairs = [kv(a, j, seg) for a in range(kvh)]
            ss = [score(qs[a], pairs[a][0]) for a in range(kvh)]
            return tuple(update(state[a], ss[a], pairs[a][1]) for a in range(kvh))

        state = lax.fori_loop(0, s_id, full, state)
        width = (half + 1) * rows
        qi = first + lax.broadcasted_iota(jnp.int32, (m4, width), 0) % sub
        ki = lax.broadcasted_iota(jnp.int32, (m4, width), 1)
        keep = ki <= qi
        for a in range(kvh):
            kj, vj = kv(a, s_id, width)
            m, l, acc = update(state[a], jnp.where(keep, score(qs[a], kj), NEG), vj)
            r = (acc / l).astype(BF)
            for b in range(g):
                ob[pl.ds(half * sub, sub), (a * g + b) * HEAD_DIM:(a * g + b + 1) * HEAD_DIM] = r[b * sub:(b + 1) * sub]

    def cols(n):
        return pl.ds(pl.multiple_of(n * tile, tile), tile)

    @pl.loop(0, 2 * nb)
    def _(i):
        for half in range(2):
            attend(i, half)

        @pl.when(i == 0)
        def _():
            load.wait()

        @pl.when(i >= 2)
        def _():
            @pl.loop(0, nt)
            def _(n):
                pass_half(i - 2, n).wait_send()

        @pl.loop(0, nt)
        def _(n):
            p = jnp.dot(ob[...], wo[:, cols(n)], preferred_element_type=F32)
            pt[i % 2, n, 0] = p[:sub]
            pt[i % 2, n, 1] = p[sub:]

            @pl.when(n > 0)
            def _():
                pass_half(i, n - 1).start()

        pass_half(i, nt - 1).start()

        @pl.loop(0, nt)
        def _(n):
            pass_half(i, n).wait_recv()
            sm[i, n] = pt[i % 2, n, core] + rc[i, n]

        @pl.when(i < nb)
        def _():
            pass_sum(i).start()

    @pl.loop(0, nb)
    def _(j):
        pass_sum(j).wait_recv()
        own = pl.ds(pl.multiple_of(j * sub, sub), sub)

        @pl.loop(0, nt)
        def _(n):
            h_ref[own, cols(n)] = (x_ref[own, cols(n)].astype(F32) + (sm[nb + j, n] + rx[j, n])).astype(BF)

    @pl.loop(0, nt)
    def _(n):
        pass_half(2 * nb - 2, n).wait_send()
        pass_half(2 * nb - 1, n).wait_send()

    @pl.loop(0, nb)
    def _(j):
        pass_sum(j).wait_send()


def attention_out(q, kvs, x, wo, cp, tp):
    t, hd = x.shape
    nb, tile = 4, 512
    sub, nt = t // nb, hd // tile
    vm = pl.BlockSpec(memory_space=pltpu.VMEM)
    dma = pltpu.SemaphoreType.DMA
    return pl.pallas_call(
        functools.partial(attn_out_body, cp=cp, tp=tp, nb=nb, tile=tile, scale=HEAD_DIM ** -0.5),
        in_specs=[vm, vm, vm, pl.BlockSpec(memory_space=pl.ANY)],
        out_specs=vm,
        out_shape=jax.ShapeDtypeStruct((t, hd), BF),
        scratch_shapes=[
            pltpu.VMEM(wo.shape, BF), pltpu.VMEM((2 * sub, wo.shape[0]), BF),
            pltpu.VMEM((2, nt, 2, sub, tile), F32), pltpu.VMEM((2 * nb, nt, sub, tile), F32),
            pltpu.VMEM((2 * nb, nt, sub, tile), F32), pltpu.VMEM((nb, nt, sub, tile), F32),
            dma, dma((2, nt)), dma((2 * nb, nt)), dma((nb,)), dma((nb,)),
        ],
        compiler_params=pltpu.CompilerParams(vmem_limit_bytes=VMEM_LIMIT, collective_id=1, has_side_effects=True),
        cost_estimate=pl.CostEstimate(flops=40_000_000_000, bytes_accessed=16_000_000, transcendentals=10_000_000),
        name='attention_out',
    )(q, kvs, x, wo)


def peer_of(c, t, d, tp):
    return {'cp': c ^ (d // tp), 'tp': t ^ (d % tp)}, (c ^ (d // tp)) * tp + (t ^ (d % tp))


def far_side(d):
    return (d >> 1) & 1


def place_of(d):
    return (d >> 2) * 2 + (d & 1)


def up_body(h_ref, tgt_ref, g_ref, u_ref, near_ref, cross_ref, pick, sb, xg, send_sem, recv_sem, *, cp, tp, cap, nf, na, wide):
    step = pl.program_id(0)
    ne = cp * tp
    c = lax.axis_index('cp')
    t = lax.axis_index('tp')

    def remote(d):
        where, _ = peer_of(c, t, d, tp)
        return pltpu.make_async_remote_copy(
            src_ref=sb.at[d], dst_ref=xg.at[far_side(d), pl.ds(place_of(d) * cap, cap)], send_sem=send_sem.at[d],
            recv_sem=recv_sem.at[d], device_id=where, device_id_type=MESH)

    @pl.when(step == 0)
    def _():
        barrier = pltpu.get_barrier_semaphore()
        for d in range(1, ne):
            pl.semaphore_signal(barrier, inc=1, device_id=peer_of(c, t, d, tp)[0], device_id_type=MESH)
        slots = lax.broadcasted_iota(jnp.int32, (cap, h_ref.shape[0]), 0)
        for d in range(ne):
            key = slots + peer_of(c, t, d, tp)[1] * cap
            hit = key == tgt_ref[0:1, :]
            for k in range(1, tgt_ref.shape[0]):
                hit = hit | (key == tgt_ref[k:k + 1, :])
            pick[pl.ds(d * cap, cap)] = jnp.where(hit, 1.0, 0.0).astype(BF)

        @pl.loop(0, h_ref.shape[1] // wide)
        def _(j):
            cols = pl.ds(pl.multiple_of(j * wide, wide), wide)
            p = jnp.dot(pick[...], h_ref[:, cols], preferred_element_type=F32).astype(BF)
            xg[0, pl.ds(0, cap), cols] = p[:cap]
            for d in range(1, ne):
                sb[d, :, cols] = p[d * cap:(d + 1) * cap]

        pl.semaphore_wait(barrier, ne - 1)
        for d in (1, 4, 5, 2, 3, 6, 7):
            remote(d).start()
        for d in (1, 4, 5):
            remote(d).wait_recv()

    @pl.when(step == na)
    def _():
        for d in (2, 3, 6, 7):
            remote(d).wait_recv()

    def hidden(x):
        gg = jnp.dot(x, g_ref[0], preferred_element_type=F32)
        uu = jnp.dot(x, u_ref[0], preferred_element_type=F32)
        return (jax.nn.silu(gg) * uu).astype(BF)

    both = (step >= na) & (step < nf)
    half = ne * cap // 2

    @pl.when(both)
    def _():
        r = hidden(xg[...].reshape(ne * cap, xg.shape[2]))
        near_ref[...] = r[:half]
        cross_ref[...] = r[half:]

    @pl.when(jnp.logical_not(both))
    def _():
        r = hidden(xg[(step >= nf).astype(jnp.int32)])

        @pl.when(step < na)
        def _():
            near_ref[...] = r

        @pl.when(step >= nf)
        def _():
            cross_ref[...] = r

    @pl.when(step == nf + na - 1)
    def _():
        for d in range(1, ne):
            remote(d).wait_send()


def expert_up(h, tgt, wg, wu, cp, tp, cap, tile, na):
    t, hd = h.shape
    ff = wg.shape[2]
    ne = cp * tp
    nf = ff // tile
    half = ne * cap // 2
    weights = lambda j: (0, 0, jnp.where(j < nf, j, j - nf))
    dma = pltpu.SemaphoreType.DMA
    return pl.pallas_call(
        functools.partial(up_body, cp=cp, tp=tp, cap=cap, nf=nf, na=na, wide=512),
        grid=(nf + na,),
        in_specs=[
            pl.BlockSpec((t, hd), lambda j: (0, 0)),
            pl.BlockSpec(tgt.shape, lambda j: (0, 0)),
            pl.BlockSpec((1, hd, tile), weights),
            pl.BlockSpec((1, hd, tile), weights),
        ],
        out_specs=[
            pl.BlockSpec((half, tile), lambda j: (0, jnp.minimum(j, nf - 1))),
            pl.BlockSpec((half, tile), lambda j: (0, jnp.where(j < nf, jnp.maximum(j, na), j - nf))),
        ],
        out_shape=[jax.ShapeDtypeStruct((half, ff), BF)] * 2,
        scratch_shapes=[
            pltpu.VMEM((ne * cap, t), BF), pltpu.VMEM((ne, cap, hd), BF), pltpu.VMEM((2, half, hd), BF),
            dma((ne,)), dma((ne,)),
        ],
        compiler_params=pltpu.CompilerParams(vmem_limit_bytes=VMEM_LIMIT, collective_id=cap + 1, has_side_effects=True),
        cost_estimate=pl.CostEstimate(flops=8 * half * hd * ff, bytes_accessed=8 * hd * ff, transcendentals=2 * half * ff),
        name='expert_up',
    )(h, tgt, wg, wu)


def down_body(near_hbm, cross_hbm, w_ref, h_ref, tgt_ref, gate_ref, y_ref, act, zs, zb, load_sem, send_sem, recv_sem, own_sem,
              *, cp, tp, cap, nt, lag):
    step = pl.program_id(0)
    ne = cp * tp
    c = lax.axis_index('cp')
    t = lax.axis_index('tp')
    me = c * tp + t

    def mine():
        return pl.ds(pl.multiple_of(me * cap, cap), cap)

    def theirs(d):
        return pl.ds((far_side(d) * ne // 2 + place_of(d)) * cap, cap)

    def remote(n, d):
        where, _ = peer_of(c, t, d, tp)
        return pltpu.make_async_remote_copy(
            src_ref=zs.at[n, theirs(d)], dst_ref=zb.at[n, mine()], send_sem=send_sem.at[n, d],
            recv_sem=recv_sem.at[n, d], device_id=where, device_id_type=MESH)

    def own(n):
        return pltpu.make_async_copy(zs.at[n, theirs(0)], zb.at[n, mine()], own_sem.at[n])

    @pl.when(step == 0)
    def _():
        half = ne * cap // 2
        loads = [pltpu.make_async_copy(near_hbm, act.at[pl.ds(0, half)], load_sem.at[0]),
                 pltpu.make_async_copy(cross_hbm, act.at[pl.ds(half, half)], load_sem.at[1])]
        for ld in loads:
            ld.start()
        barrier = pltpu.get_barrier_semaphore()
        for d in range(1, ne):
            pl.semaphore_signal(barrier, inc=1, device_id=peer_of(c, t, d, tp)[0], device_id_type=MESH)
        pl.semaphore_wait(barrier, ne - 1)
        for ld in loads:
            ld.wait()

    @pl.when((step >= 1) & (step <= nt))
    def _():
        for d in (2, 3, 6, 7, 4, 5, 1):
            remote(step - 1, d).start()
        own(step - 1).start()

    @pl.when(step < nt)
    def _():
        zs[step] = jnp.dot(act[...], w_ref[0], preferred_element_type=F32).astype(BF)

    @pl.when(step >= lag)
    def _():
        n = step - lag
        own(n).wait()
        for d in range(1, ne):
            remote(n, d).wait_recv()
        slots = lax.broadcasted_iota(jnp.int32, (tgt_ref.shape[0], ne * cap), 1)
        z = zb[n]
        acc = h_ref[...].astype(F32)
        zsum = None
        for k in range(tgt_ref.shape[1]):
            pick = (slots == tgt_ref[:, k:k + 1]).astype(BF)
            zk = gate_ref[:, k:k + 1] * jnp.dot(pick, z, preferred_element_type=F32)
            zsum = zk if zsum is None else zsum + zk
        y_ref[...] = (acc + zsum).astype(BF)
        for d in range(1, ne):
            remote(n, d).wait_send()


def expert_down(near, cross, wd, h, tgt, gates, cp, tp, cap, tile, lag):
    half, ff = near.shape
    r = 2 * half
    t, hd = h.shape
    kk = tgt.shape[1]
    ne = cp * tp
    nt = hd // tile
    late = lambda j: (0, jnp.maximum(j - lag, 0))
    dma = pltpu.SemaphoreType.DMA
    return pl.pallas_call(
        functools.partial(down_body, cp=cp, tp=tp, cap=cap, nt=nt, lag=lag),
        grid=(nt + lag,),
        in_specs=[
            pl.BlockSpec(memory_space=pl.ANY),
            pl.BlockSpec(memory_space=pl.ANY),
            pl.BlockSpec((1, ff, tile), lambda j: (0, 0, jnp.minimum(j, nt - 1))),
            pl.BlockSpec((t, tile), late),
            pl.BlockSpec((t, kk), lambda j: (0, 0)),
            pl.BlockSpec((t, kk), lambda j: (0, 0)),
        ],
        out_specs=pl.BlockSpec((t, tile), late),
        out_shape=jax.ShapeDtypeStruct((t, hd), BF),
        scratch_shapes=[
            pltpu.VMEM((r, ff), BF),
            pltpu.VMEM((nt, r, tile), BF),
            pltpu.VMEM((nt, r, tile), BF),
            dma((2,)), dma((nt, ne)), dma((nt, ne)), dma((nt,)),
        ],
        compiler_params=pltpu.CompilerParams(vmem_limit_bytes=VMEM_LIMIT, collective_id=cap, has_side_effects=True),
        cost_estimate=pl.CostEstimate(flops=2 * r * hd * ff, bytes_accessed=2 * hd * ff, transcendentals=0),
        name='expert_down',
    )(near, cross, wd, h, tgt, gates)


def solution(mesh):
    cp = mesh.shape['cp']
    tp = mesh.shape['tp']
    ne = cp * tp
    rows_spec = P(('dp', 'cp', 'tp'), None)
    exp_spec = P(('cp', 'tp'), None, None)

    def local(x, idx, gates, wq, wk, wv, wo, w1g, w1u, w2):
        t, hd = x.shape
        kk = idx.shape[1]

        ea = idx.reshape(-1)
        onehot = (ea[:, None] == jnp.arange(ne)[None, :]).astype(jnp.int32)
        cum = jnp.cumsum(onehot, axis=0)
        slot = (jnp.sum(cum * onehot, axis=1) - 1).reshape(t, kk)
        cnt = jnp.broadcast_to(jnp.max(cum[-1]), (8, 128))
        q, kvs, top = project_qkv(x, cnt, wq, wk, wv, cp, tp)
        fullest = top[0, 0]
        h = attention_out(q, kvs, x, wo, cp, tp)

        def moe(cap):
            def run(h, idx, slot, gates, w1g, w1u, w2):
                tgt = idx * cap + slot
                near, cross = expert_up(h, tgt.T, w1g, w1u, cp, tp, cap, 256, 16)
                return expert_down(near, cross, w2, h, tgt, gates, cp, tp, cap, 256, 4)
            return run

        caps = (2 * t // ne, 3 * t // ne, 4 * t // ne)
        tier = (fullest > caps[0]).astype(jnp.int32) + (fullest > caps[1]).astype(jnp.int32)
        return lax.switch(tier, [moe(cap) for cap in caps], h, idx, slot, gates, w1g, w1u, w2)

    return jax.shard_map(local, mesh=mesh, in_specs=(rows_spec, rows_spec, rows_spec, P(None, 'tp'), P(None, 'tp'), P(None, 'tp'), P('tp', None), exp_spec, exp_spec, exp_spec), out_specs=rows_spec, check_vma=False)
```

```python
import functools

import jax
import jax.numpy as jnp
from jax import lax
from jax.experimental import pallas as pl
from jax.experimental.pallas import tpu as pltpu
from jax.sharding import PartitionSpec as P

HEAD_DIM = 128
NEG = -1e30
LOG2E = 1.4426950408889634
MESH = pl.DeviceIdType.MESH
BF = jnp.bfloat16
F32 = jnp.float32
VMEM_LIMIT = 60 * 1024 * 1024


def qkv_body(x_ref, cnt_ref, wq_hbm, wk_hbm, wv_hbm, q_ref, kv_ref, top_ref, wq, wk, wv, near, far, cnts,
             load_sem, psend, precv, xsend, xrecv, fsend, frecv, ksend, krecv, csend, crecv, *, cp, tp, ch):
    c = lax.axis_index('cp')
    t = lax.axis_index('tp')
    rows, hd = x_ref.shape
    part = rows // ch
    wide = q_ref.shape[1]
    kw = wk.shape[1]
    partner, across, other = {'tp': t ^ 1}, {'tp': t ^ 2}, {'cp': 1 - c}

    loads = [pltpu.make_async_copy(s, d, load_sem.at[i]) for i, (s, d) in enumerate(((wk_hbm, wk), (wv_hbm, wv), (wq_hbm, wq)))]
    for ld in loads:
        ld.start()

    def peer(d):
        return {'cp': c ^ (d // tp), 'tp': t ^ (d % tp)}

    barrier = pltpu.get_barrier_semaphore()
    for d in range(1, cp * tp):
        pl.semaphore_signal(barrier, inc=1, device_id=peer(d), device_id_type=MESH)
    pl.semaphore_wait(barrier, cp * tp - 1)

    def copy(src, dst, ss, rs, where):
        return pltpu.make_async_remote_copy(src_ref=src, dst_ref=dst, send_sem=ss, recv_sem=rs, device_id=where, device_id_type=MESH)

    out = [copy(x_ref.at[pl.ds(i * part, part)], far.at[i, 0], xsend.at[i], xrecv.at[i], across) for i in range(ch)]
    fwd = [copy(far.at[i, 0], far.at[i, 1], fsend.at[i], frecv.at[i], partner) for i in range(ch)]
    side = copy(x_ref, near, psend, precv, partner)
    count = [copy(cnt_ref, cnts.at[d], csend.at[d], crecv.at[d], peer(d)) for d in range(1, cp * tp)]
    for cpy in out:
        cpy.start()
    side.start()
    for cpy in count:
        cpy.start()

    def keys(n, first, size):
        sl = (c, pl.ds(pl.multiple_of(first, part), size))
        return copy(kv_ref.at[sl], kv_ref.at[sl], ksend.at[n], krecv.at[n], other)

    def project(xv, pieces, sends):
        def put(ref, val, col, width):
            for a, size, first in pieces:
                ref[pl.ds(pl.multiple_of(first, part), size), pl.ds(col, width)] = val[a:a + size].astype(BF)

        mine = kv_ref.at[c]
        put(mine, jnp.dot(xv, wk[...], preferred_element_type=F32), 0, kw)
        put(mine, jnp.dot(xv, wv[...], preferred_element_type=F32), kw, kw)

        def qtile(j):
            col = pl.multiple_of(j * kw, kw)
            put(q_ref, jnp.dot(xv, wq[:, pl.ds(col, kw)], preferred_element_type=F32), col, kw)

        qtile(0)
        for s in sends:
            s.start()

        @pl.loop(1, wide // kw)
        def _(j):
            qtile(j)

    for ld in loads:
        ld.wait()
    kcopies = []
    k0 = keys(0, t * rows, rows)
    kcopies.append(k0)
    project(x_ref[...], ((0, rows, t * rows),), (k0,))
    side.wait_recv()
    k1 = keys(1, (t ^ 1) * rows, rows)
    kcopies.append(k1)
    project(near[...], ((0, rows, (t ^ 1) * rows),), (k1,))
    for i in range(ch):
        out[i].wait_recv()
        fwd[i].start()
        fwd[i].wait_recv()
        r2 = (t ^ 2) * rows + i * part
        r3 = (t ^ 3) * rows + i * part
        ks = (keys(2 + 2 * i, r2, part), keys(3 + 2 * i, r3, part))
        kcopies.extend(ks)
        project(far[i].reshape(2 * part, hd), ((0, part, r2), (part, part, r3)), ks)
    top = cnt_ref[...]
    for d in range(1, cp * tp):
        count[d - 1].wait()
        top = jnp.maximum(top, cnts[d])
    top_ref[...] = top

    def keys_in(n, first, size):
        sl = (1 - c, pl.ds(pl.multiple_of(first, part), size))
        return copy(kv_ref.at[sl], kv_ref.at[sl], ksend.at[n], krecv.at[n], other)

    keys_in(0, t * rows, rows).wait_recv()
    keys_in(1, (t ^ 1) * rows, rows).wait_recv()
    for i in range(ch):
        keys_in(2 + 2 * i, (t ^ 2) * rows + i * part, part).wait_recv()
        keys_in(3 + 2 * i, (t ^ 3) * rows + i * part, part).wait_recv()
    for kc in kcopies:
        kc.wait_send()
    side.wait_send()
    for i in range(ch):
        out[i].wait_send()
        fwd[i].wait_send()


def project_qkv(x, cnt, wq, wk, wv, cp, tp):
    t, hd = x.shape
    n = t * tp
    wide, kw = wq.shape[1], wk.shape[1]
    ch = 4
    vm = pl.BlockSpec(memory_space=pltpu.VMEM)
    hbm = pl.BlockSpec(memory_space=pl.ANY)
    dma = pltpu.SemaphoreType.DMA
    return pl.pallas_call(
        functools.partial(qkv_body, cp=cp, tp=tp, ch=ch),
        in_specs=[vm, vm, hbm, hbm, hbm],
        out_specs=[vm, vm, vm],
        out_shape=[jax.ShapeDtypeStruct((n, wide), BF), jax.ShapeDtypeStruct((cp, n, 2 * kw), BF), jax.ShapeDtypeStruct(cnt.shape, cnt.dtype)],
        scratch_shapes=[
            pltpu.VMEM(wq.shape, BF), pltpu.VMEM(wk.shape, BF), pltpu.VMEM(wv.shape, BF),
            pltpu.VMEM((t, hd), BF), pltpu.VMEM((ch, 2, t // ch, hd), BF), pltpu.VMEM((cp * tp,) + cnt.shape, cnt.dtype),
            dma((3,)), dma, dma, dma((ch,)), dma((ch,)), dma((ch,)), dma((ch,)),
            dma((2 + 2 * ch,)), dma((2 + 2 * ch,)), dma((cp * tp,)), dma((cp * tp,)),
        ],
        compiler_params=pltpu.CompilerParams(vmem_limit_bytes=VMEM_LIMIT, collective_id=0, has_side_effects=True),
        cost_estimate=pl.CostEstimate(flops=2 * n * hd * (wide + 2 * kw), bytes_accessed=20_000_000, transcendentals=0),
        name='project_qkv',
    )(x, cnt, wq, wk, wv)


def attn_out_body(q_ref, kv_ref, x_ref, wo_hbm, h_ref, wo, ob, pt, rc, sm, rx,
                  load_sem, dsend, drecv, xsend, xrecv, *, cp, tp, nb, tile, scale):
    c = lax.axis_index('cp')
    t = lax.axis_index('tp')
    core, side = t % 2, t // 2
    rows, hd = x_ref.shape
    seg = 2 * rows
    sub = rows // nb
    nt = hd // tile
    heads = q_ref.shape[1] // HEAD_DIM
    kvh = kv_ref.shape[2] // (2 * HEAD_DIM)
    g = heads // kvh
    cc = scale * LOG2E

    load = pltpu.make_async_copy(wo_hbm, wo, load_sem)
    load.start()
    partner, across = {'tp': t ^ 1}, {'tp': t ^ 2}
    barrier = pltpu.get_barrier_semaphore()
    for where in (partner, across):
        pl.semaphore_signal(barrier, inc=1, device_id=where, device_id_type=MESH)
    pl.semaphore_wait(barrier, 2)

    def pass_half(i, n):
        return pltpu.make_async_remote_copy(
            src_ref=pt.at[i % 2, n, 1 - core], dst_ref=rc.at[i, n], send_sem=dsend.at[i % 2, n], recv_sem=drecv.at[i, n],
            device_id=partner, device_id_type=MESH)

    def pass_sum(i):
        return pltpu.make_async_remote_copy(
            src_ref=sm.at[i], dst_ref=rx.at[i], send_sem=xsend.at[i], recv_sem=xrecv.at[i],
            device_id=across, device_id_type=MESH)

    def score(q, kj):
        return lax.dot_general(q, kj, (((1,), (1,)), ((), ())), preferred_element_type=F32)

    def update(state, s, vj):
        m, l, acc = state
        mn = jnp.maximum(m, jnp.max(s, axis=-1, keepdims=True))
        w = jnp.exp2((s - mn) * cc)
        a = jnp.exp2((m - mn) * cc)
        l = l * a + jnp.sum(w, axis=-1, keepdims=True)
        acc = acc * a + jnp.dot(w.astype(BF), vj, preferred_element_type=F32)
        return mn, l, acc

    def block(s_id, width):
        src = jnp.where(s_id < cp, s_id, 2 * cp - 1 - s_id)
        return src, pl.ds(pl.multiple_of(jnp.where(s_id < cp, 0, seg), seg), width)

    def attend(i, half):
        place = jnp.where(i < nb, 1 - side, side)
        s_id = jnp.where(place == 0, c, 2 * cp - 1 - c)
        first = half * rows + (i % nb) * sub
        qrows = pl.ds(pl.multiple_of(place * seg + first, sub), sub)
        m4 = g * sub
        qs = [jnp.concatenate([q_ref[qrows, (a * g + b) * HEAD_DIM:(a * g + b + 1) * HEAD_DIM] for b in range(g)], axis=0)
              for a in range(kvh)]
        state = tuple((jnp.full((m4, 1), NEG, F32), jnp.zeros((m4, 1), F32), jnp.zeros((m4, HEAD_DIM), F32)) for _ in range(kvh))

        def kv(a, s, width):
            src, sl = block(s, width)
            return (kv_ref[src, sl, a * HEAD_DIM:(a + 1) * HEAD_DIM],
                    kv_ref[src, sl, (kvh + a) * HEAD_DIM:(kvh + a + 1) * HEAD_DIM])

        def full(j, state):
            pairs = [kv(a, j, seg) for a in range(kvh)]
            ss = [score(qs[a], pairs[a][0]) for a in range(kvh)]
            return tuple(update(state[a], ss[a], pairs[a][1]) for a in range(kvh))

        state = lax.fori_loop(0, s_id, full, state)
        width = (half + 1) * rows
        qi = first + lax.broadcasted_iota(jnp.int32, (m4, width), 0) % sub
        ki = lax.broadcasted_iota(jnp.int32, (m4, width), 1)
        keep = ki <= qi
        for a in range(kvh):
            kj, vj = kv(a, s_id, width)
            m, l, acc = update(state[a], jnp.where(keep, score(qs[a], kj), NEG), vj)
            r = (acc / l).astype(BF)
            for b in range(g):
                ob[pl.ds(half * sub, sub), (a * g + b) * HEAD_DIM:(a * g + b + 1) * HEAD_DIM] = r[b * sub:(b + 1) * sub]

    def cols(n):
        return pl.ds(pl.multiple_of(n * tile, tile), tile)

    @pl.loop(0, 2 * nb)
    def _(i):
        for half in range(2):
            attend(i, half)

        @pl.when(i == 0)
        def _():
            load.wait()

        @pl.when(i >= 2)
        def _():
            @pl.loop(0, nt)
            def _(n):
                pass_half(i - 2, n).wait_send()

        @pl.loop(0, nt)
        def _(n):
            p = jnp.dot(ob[...], wo[:, cols(n)], preferred_element_type=F32)
            pt[i % 2, n, 0] = p[:sub]
            pt[i % 2, n, 1] = p[sub:]

            @pl.when(n > 0)
            def _():
                pass_half(i, n - 1).start()

        pass_half(i, nt - 1).start()

        @pl.loop(0, nt)
        def _(n):
            pass_half(i, n).wait_recv()
            sm[i, n] = pt[i % 2, n, core] + rc[i, n]

        @pl.when(i < nb)
        def _():
            pass_sum(i).start()

    @pl.loop(0, nb)
    def _(j):
        pass_sum(j).wait_recv()
        own = pl.ds(pl.multiple_of(j * sub, sub), sub)

        @pl.loop(0, nt)
        def _(n):
            h_ref[own, cols(n)] = (x_ref[own, cols(n)].astype(F32) + (sm[nb + j, n] + rx[j, n])).astype(BF)

    @pl.loop(0, nt)
    def _(n):
        pass_half(2 * nb - 2, n).wait_send()
        pass_half(2 * nb - 1, n).wait_send()

    @pl.loop(0, nb)
    def _(j):
        pass_sum(j).wait_send()


def attention_out(q, kvs, x, wo, cp, tp):
    t, hd = x.shape
    nb, tile = 4, 512
    sub, nt = t // nb, hd // tile
    vm = pl.BlockSpec(memory_space=pltpu.VMEM)
    dma = pltpu.SemaphoreType.DMA
    return pl.pallas_call(
        functools.partial(attn_out_body, cp=cp, tp=tp, nb=nb, tile=tile, scale=HEAD_DIM ** -0.5),
        in_specs=[vm, vm, vm, pl.BlockSpec(memory_space=pl.ANY)],
        out_specs=vm,
        out_shape=jax.ShapeDtypeStruct((t, hd), BF),
        scratch_shapes=[
            pltpu.VMEM(wo.shape, BF), pltpu.VMEM((2 * sub, wo.shape[0]), BF),
            pltpu.VMEM((2, nt, 2, sub, tile), F32), pltpu.VMEM((2 * nb, nt, sub, tile), F32),
            pltpu.VMEM((2 * nb, nt, sub, tile), F32), pltpu.VMEM((nb, nt, sub, tile), F32),
            dma, dma((2, nt)), dma((2 * nb, nt)), dma((nb,)), dma((nb,)),
        ],
        compiler_params=pltpu.CompilerParams(vmem_limit_bytes=VMEM_LIMIT, collective_id=1, has_side_effects=True),
        cost_estimate=pl.CostEstimate(flops=40_000_000_000, bytes_accessed=16_000_000, transcendentals=10_000_000),
        name='attention_out',
    )(q, kvs, x, wo)


def peer_of(c, t, d, tp):
    return {'cp': c ^ (d // tp), 'tp': t ^ (d % tp)}, (c ^ (d // tp)) * tp + (t ^ (d % tp))


def far_side(d):
    return (d >> 1) & 1


def place_of(d):
    return (d >> 2) * 2 + (d & 1)


def up_body(h_ref, tgt_ref, g_ref, u_ref, near_ref, cross_ref, pick, sb, xg, via, send_sem, recv_sem, hop_send, hop_recv, *, cp, tp, cap, nf, na, wide):
    step = pl.program_id(0)
    ne = cp * tp
    c = lax.axis_index('cp')
    t = lax.axis_index('tp')

    def remote(d):
        where, _ = peer_of(c, t, d, tp)
        return pltpu.make_async_remote_copy(
            src_ref=sb.at[d], dst_ref=xg.at[far_side(d), pl.ds(place_of(d) * cap, cap)], send_sem=send_sem.at[d],
            recv_sem=recv_sem.at[d], device_id=where, device_id_type=MESH)

    def hop(d):
        return pltpu.make_async_remote_copy(
            src_ref=sb.at[d], dst_ref=via.at[d - 6], send_sem=hop_send.at[d - 6], recv_sem=hop_recv.at[d - 6],
            device_id={'tp': t ^ 2}, device_id_type=MESH)

    def pass_on(d):
        return pltpu.make_async_remote_copy(
            src_ref=via.at[d - 6], dst_ref=xg.at[far_side(d), pl.ds(place_of(d) * cap, cap)], send_sem=send_sem.at[d],
            recv_sem=recv_sem.at[d], device_id={'cp': 1 - c, 'tp': t ^ (d - 6)}, device_id_type=MESH)

    @pl.when(step == 0)
    def _():
        barrier = pltpu.get_barrier_semaphore()
        for d in range(1, ne):
            pl.semaphore_signal(barrier, inc=1, device_id=peer_of(c, t, d, tp)[0], device_id_type=MESH)
        slots = lax.broadcasted_iota(jnp.int32, (cap, h_ref.shape[0]), 0)
        for d in range(ne):
            key = slots + peer_of(c, t, d, tp)[1] * cap
            hit = key == tgt_ref[0:1, :]
            for k in range(1, tgt_ref.shape[0]):
                hit = hit | (key == tgt_ref[k:k + 1, :])
            pick[pl.ds(d * cap, cap)] = jnp.where(hit, 1.0, 0.0).astype(BF)

        @pl.loop(0, h_ref.shape[1] // wide)
        def _(j):
            cols = pl.ds(pl.multiple_of(j * wide, wide), wide)
            p = jnp.dot(pick[...], h_ref[:, cols], preferred_element_type=F32).astype(BF)
            xg[0, pl.ds(0, cap), cols] = p[:cap]
            for d in range(1, ne):
                sb[d, :, cols] = p[d * cap:(d + 1) * cap]

        pl.semaphore_wait(barrier, ne - 1)
        for d in (6, 7):
            hop(d).start()
        for d in (4, 5, 1):
            remote(d).start()
        for d in (6, 7):
            hop(d).wait_send()
        for d in (2, 3):
            remote(d).start()
        for d in (6, 7):
            hop(d).wait_recv()
            pass_on(d).start()
        for d in (1, 4, 5):
            remote(d).wait_recv()

    @pl.when(step == na)
    def _():
        for d in (2, 3):
            remote(d).wait_recv()
        for d in (6, 7):
            pass_on(d).wait_recv()

    def hidden(x):
        gg = jnp.dot(x, g_ref[0], preferred_element_type=F32)
        uu = jnp.dot(x, u_ref[0], preferred_element_type=F32)
        return (jax.nn.silu(gg) * uu).astype(BF)

    both = (step >= na) & (step < nf)
    half = ne * cap // 2

    @pl.when(both)
    def _():
        r = hidden(xg[...].reshape(ne * cap, xg.shape[2]))
        near_ref[...] = r[:half]
        cross_ref[...] = r[half:]

    @pl.when(jnp.logical_not(both))
    def _():
        r = hidden(xg[(step >= nf).astype(jnp.int32)])

        @pl.when(step < na)
        def _():
            near_ref[...] = r

        @pl.when(step >= nf)
        def _():
            cross_ref[...] = r

    @pl.when(step == nf + na - 1)
    def _():
        for d in range(1, 6):
            remote(d).wait_send()
        for d in (6, 7):
            pass_on(d).wait_send()


def expert_up(h, tgt, wg, wu, cp, tp, cap, tile, na):
    t, hd = h.shape
    ff = wg.shape[2]
    ne = cp * tp
    nf = ff // tile
    half = ne * cap // 2
    weights = lambda j: (0, 0, jnp.where(j < nf, j, j - nf))
    dma = pltpu.SemaphoreType.DMA
    return pl.pallas_call(
        functools.partial(up_body, cp=cp, tp=tp, cap=cap, nf=nf, na=na, wide=512),
        grid=(nf + na,),
        in_specs=[
            pl.BlockSpec((t, hd), lambda j: (0, 0)),
            pl.BlockSpec(tgt.shape, lambda j: (0, 0)),
            pl.BlockSpec((1, hd, tile), weights),
            pl.BlockSpec((1, hd, tile), weights),
        ],
        out_specs=[
            pl.BlockSpec((half, tile), lambda j: (0, jnp.minimum(j, nf - 1))),
            pl.BlockSpec((half, tile), lambda j: (0, jnp.where(j < nf, jnp.maximum(j, na), j - nf))),
        ],
        out_shape=[jax.ShapeDtypeStruct((half, ff), BF)] * 2,
        scratch_shapes=[
            pltpu.VMEM((ne * cap, t), BF), pltpu.VMEM((ne, cap, hd), BF), pltpu.VMEM((2, half, hd), BF),
            pltpu.VMEM((2, cap, hd), BF), dma((ne,)), dma((ne,)), dma((2,)), dma((2,)),
        ],
        compiler_params=pltpu.CompilerParams(vmem_limit_bytes=VMEM_LIMIT, collective_id=cap + 1, has_side_effects=True),
        cost_estimate=pl.CostEstimate(flops=8 * half * hd * ff, bytes_accessed=8 * hd * ff, transcendentals=2 * half * ff),
        name='expert_up',
    )(h, tgt, wg, wu)


def down_body(near_hbm, cross_hbm, w_ref, h_ref, tgt_ref, gate_ref, y_ref, act, zs, zb, load_sem, send_sem, recv_sem, own_sem,
              *, cp, tp, cap, nt, lag):
    step = pl.program_id(0)
    ne = cp * tp
    c = lax.axis_index('cp')
    t = lax.axis_index('tp')
    me = c * tp + t

    def mine():
        return pl.ds(pl.multiple_of(me * cap, cap), cap)

    def theirs(d):
        return pl.ds((far_side(d) * ne // 2 + place_of(d)) * cap, cap)

    def remote(n, d):
        where, _ = peer_of(c, t, d, tp)
        return pltpu.make_async_remote_copy(
            src_ref=zs.at[n, theirs(d)], dst_ref=zb.at[n, mine()], send_sem=send_sem.at[n, d],
            recv_sem=recv_sem.at[n, d], device_id=where, device_id_type=MESH)

    def own(n):
        return pltpu.make_async_copy(zs.at[n, theirs(0)], zb.at[n, mine()], own_sem.at[n])

    @pl.when(step == 0)
    def _():
        half = ne * cap // 2
        loads = [pltpu.make_async_copy(near_hbm, act.at[pl.ds(0, half)], load_sem.at[0]),
                 pltpu.make_async_copy(cross_hbm, act.at[pl.ds(half, half)], load_sem.at[1])]
        for ld in loads:
            ld.start()
        barrier = pltpu.get_barrier_semaphore()
        for d in range(1, ne):
            pl.semaphore_signal(barrier, inc=1, device_id=peer_of(c, t, d, tp)[0], device_id_type=MESH)
        pl.semaphore_wait(barrier, ne - 1)
        for ld in loads:
            ld.wait()

    @pl.when((step >= 1) & (step <= nt))
    def _():
        for d in (2, 3, 6, 7, 4, 5, 1):
            remote(step - 1, d).start()
        own(step - 1).start()

    @pl.when(step < nt)
    def _():
        zs[step] = jnp.dot(act[...], w_ref[0], preferred_element_type=F32).astype(BF)

    @pl.when(step >= lag)
    def _():
        n = step - lag
        own(n).wait()
        for d in range(1, ne):
            remote(n, d).wait_recv()
        slots = lax.broadcasted_iota(jnp.int32, (tgt_ref.shape[0], ne * cap), 1)
        z = zb[n]
        acc = h_ref[...].astype(F32)
        zsum = None
        for k in range(tgt_ref.shape[1]):
            pick = (slots == tgt_ref[:, k:k + 1]).astype(BF)
            zk = gate_ref[:, k:k + 1] * jnp.dot(pick, z, preferred_element_type=F32)
            zsum = zk if zsum is None else zsum + zk
        y_ref[...] = (acc + zsum).astype(BF)
        for d in range(1, ne):
            remote(n, d).wait_send()


def expert_down(near, cross, wd, h, tgt, gates, cp, tp, cap, tile, lag):
    half, ff = near.shape
    r = 2 * half
    t, hd = h.shape
    kk = tgt.shape[1]
    ne = cp * tp
    nt = hd // tile
    late = lambda j: (0, jnp.maximum(j - lag, 0))
    dma = pltpu.SemaphoreType.DMA
    return pl.pallas_call(
        functools.partial(down_body, cp=cp, tp=tp, cap=cap, nt=nt, lag=lag),
        grid=(nt + lag,),
        in_specs=[
            pl.BlockSpec(memory_space=pl.ANY),
            pl.BlockSpec(memory_space=pl.ANY),
            pl.BlockSpec((1, ff, tile), lambda j: (0, 0, jnp.minimum(j, nt - 1))),
            pl.BlockSpec((t, tile), late),
            pl.BlockSpec((t, kk), lambda j: (0, 0)),
            pl.BlockSpec((t, kk), lambda j: (0, 0)),
        ],
        out_specs=pl.BlockSpec((t, tile), late),
        out_shape=jax.ShapeDtypeStruct((t, hd), BF),
        scratch_shapes=[
            pltpu.VMEM((r, ff), BF),
            pltpu.VMEM((nt, r, tile), BF),
            pltpu.VMEM((nt, r, tile), BF),
            dma((2,)), dma((nt, ne)), dma((nt, ne)), dma((nt,)),
        ],
        compiler_params=pltpu.CompilerParams(vmem_limit_bytes=VMEM_LIMIT, collective_id=cap, has_side_effects=True),
        cost_estimate=pl.CostEstimate(flops=2 * r * hd * ff, bytes_accessed=2 * hd * ff, transcendentals=0),
        name='expert_down',
    )(near, cross, wd, h, tgt, gates)


def solution(mesh):
    cp = mesh.shape['cp']
    tp = mesh.shape['tp']
    ne = cp * tp
    rows_spec = P(('dp', 'cp', 'tp'), None)
    exp_spec = P(('cp', 'tp'), None, None)

    def local(x, idx, gates, wq, wk, wv, wo, w1g, w1u, w2):
        t, hd = x.shape
        kk = idx.shape[1]

        ea = idx.reshape(-1)
        onehot = (ea[:, None] == jnp.arange(ne)[None, :]).astype(jnp.int32)
        cum = jnp.cumsum(onehot, axis=0)
        slot = (jnp.sum(cum * onehot, axis=1) - 1).reshape(t, kk)
        cnt = jnp.broadcast_to(jnp.max(cum[-1]), (8, 128))
        q, kvs, top = project_qkv(x, cnt, wq, wk, wv, cp, tp)
        fullest = top[0, 0]
        h = attention_out(q, kvs, x, wo, cp, tp)

        def moe(cap):
            def run(h, idx, slot, gates, w1g, w1u, w2):
                tgt = idx * cap + slot
                near, cross = expert_up(h, tgt.T, w1g, w1u, cp, tp, cap, 256, 16)
                return expert_down(near, cross, w2, h, tgt, gates, cp, tp, cap, 256, 4)
            return run

        caps = (2 * t // ne, 3 * t // ne, 4 * t // ne)
        tier = (fullest > caps[0]).astype(jnp.int32) + (fullest > caps[1]).astype(jnp.int32)
        return lax.switch(tier, [moe(cap) for cap in caps], h, idx, slot, gates, w1g, w1u, w2)

    return jax.shard_map(local, mesh=mesh, in_specs=(rows_spec, rows_spec, rows_spec, P(None, 'tp'), P(None, 'tp'), P(None, 'tp'), P('tp', None), exp_spec, exp_spec, exp_spec), out_specs=rows_spec, check_vma=False)
```
